32 devices in a mesh: subj: 8 (over z, y), slab: 4 (over x, core).
Axes of the slice: x: 2, y: 2, z: 4, core: 2. Of those that a mesh axis runs over, the one named last changes fastest.
Arguments:
- fod: bfloat16 [32, 45, 2048], P('subj', None, 'slab'), may hold values from -24 to 24
- rotation: bfloat16 [32, 45, 45, 2048], P('subj', None, None, 'slab'), may hold values from -0.875 to 0.875
- modulation: float32 [32, 2048], P('subj', 'slab'), may hold values from 0.3 to 3
- subject_ids: int32 [32], P('subj'), may hold values from 0 to 31, each once
- subject_weight: float32 [32], replicated, may hold values from 0.5 to 2
- voxel_cell_index: int32 [2048], P('slab'), may hold values from 0 to 1023, as said below
Outputs:
- template: bfloat16 [45, 4096], replicated
The draws below stay inside these ranges and needn't reach their ends.
Inputs may be any that keep to these rules, and one draw needn't show every extreme that they name: `voxel_cell_index`: within each aligned block of 512 entries (one slab's masked voxels) the cell numbers are distinct and increasing.
All inputs are finite; a program needn't handle non-finite values.
Results may differ from the reference program's by a relative error of at most 0.001.
Values may be sent and summed in bfloat16 or wider, within the bound.
No kernel may reach another device: no remote copies, remote signals or barrier semaphores. Data moves between devices by JAX's collectives and lax.ppermute only.
A program may use at most 64 MiB of HBM per device.

```python
import math
import jax
import jax.numpy as jnp
from jax import lax

COEF = 45
VOX_DEV = 512
GRID_DEV = 1024
SUBJECTS = 32
MASKED_VOXELS = 2048
N_SLAB = 4


def draw_voxel_cell_index(key, part):
    keys = jax.random.split(jax.random.fold_in(key, 7), N_SLAB)

    def single_slab_block(slab_key):
        order = jax.random.permutation(slab_key, GRID_DEV)
        return jnp.sort(order[:VOX_DEV])
    blocks = jax.vmap(single_slab_block)(keys)
    return blocks.reshape(VOX_DEV * N_SLAB).astype(jnp.int32)


def block_scale(own_key, dims, shards, low, high):
    loudness = 1.0
    for dim, blocks in shards:
        draws = jax.random.uniform(jax.random.fold_in(jax.random.fold_in(own_key, 6), dim), (blocks,), jnp.float32, low / len(shards), high / len(shards))
        loudness = loudness * jnp.repeat(jnp.exp(draws), dims[dim] // blocks).reshape((-1,) + (1,) * (len(dims) - 1 - dim))
    return loudness


def bell_draw(rng, extent, width, bound, shards=(), kind=jnp.bfloat16):
    factor_of = block_scale(rng, extent, shards, -0.22, 0.18) if shards else 1.0
    values = jax.random.normal(rng, extent, jnp.float32) * width * factor_of
    return jnp.minimum(jnp.maximum(values, -bound), bound).astype(kind)


def setup_inputs(seed: int = 0) -> dict:
    seeds = jax.random.split(jax.random.key(seed), 7)
    fod = bell_draw(seeds[0], (SUBJECTS, COEF, MASKED_VOXELS), 4.0, 24.0, ((0, 8), (2, 4)))
    rotation = bell_draw(seeds[1], (SUBJECTS, COEF, COEF, MASKED_VOXELS), COEF ** -0.5, 0.875, ((0, 8), (3, 4)))
    modulation = jnp.clip(jnp.exp(math.log(3.0) - 2.3025851 * jax.random.uniform(seeds[2], (SUBJECTS, MASKED_VOXELS), jnp.float32) ** block_scale(seeds[2], (SUBJECTS, MASKED_VOXELS), ((0, 8), (1, 4)), -0.2, 0.2)), 0.3, 3.0)
    subject_ids = jax.random.permutation(seeds[3], SUBJECTS).astype(jnp.int32)
    subject_weight = jnp.clip(jnp.exp(jax.random.uniform(seeds[4], (SUBJECTS,), jnp.float32, math.log(0.5), math.log(2.0))), 0.5, 2.0)
    voxel_cell_index = draw_voxel_cell_index(jax.random.fold_in(seeds[6], 71), 0)
    return {"fod": fod, "rotation": rotation, "modulation": modulation, "subject_ids": subject_ids, "subject_weight": subject_weight, "voxel_cell_index": voxel_cell_index}


def reference(fod, rotation, modulation, subject_ids, subject_weight, voxel_cell_index):
    selected_cells = subject_weight[subject_ids]
    weight = modulation * selected_cells[:, None]

    def accumulate_weighted(total, items):
        rot_one, fod_one, weight_one = items
        rotated_coefficients = jnp.einsum("ckv,kv->cv", rot_one.astype(jnp.float32), fod_one.astype(jnp.float32))
        return total + rotated_coefficients * weight_one[None, :], None

    start = jnp.zeros((COEF, MASKED_VOXELS), jnp.float32)
    numer, unused = lax.scan(accumulate_weighted, start, (rotation, fod, weight))
    denom = jnp.sum(weight, axis=0)
    average = (numer / denom[None, :]).astype(jnp.bfloat16)
    slab_lookup = (jnp.arange(MASKED_VOXELS, dtype=jnp.int32) // VOX_DEV).astype(jnp.int32)
    cells = (voxel_cell_index + slab_lookup * GRID_DEV).astype(jnp.int32)
    template = jnp.zeros((COEF, GRID_DEV * N_SLAB), jnp.bfloat16)
    return template.at[:, cells].set(average)
```

```python
import jax
import jax.numpy as jnp
from jax import lax
from jax.sharding import PartitionSpec as P

GRID_DEV = 1024


def exchange(value, axis, size, bit):
    return lax.ppermute(value, axis, [(i, i ^ bit) for i in range(size)])


def butterfly_sum(value, axis, size):
    if size & (size - 1):
        return lax.psum(value, axis)
    bit = 1
    while bit < size:
        value = value + exchange(value, axis, size, bit)
        bit *= 2
    return value


def butterfly_gather(value, axis, size):
    if size & (size - 1):
        return lax.all_gather(value, axis, axis=1, tiled=True)
    index = lax.axis_index(axis)
    width = value.shape[1]
    bit = size // 2
    while bit:
        other = exchange(value, axis, size, bit)
        low = (index & bit) == 0
        first, second = jnp.where(low, value, other), jnp.where(low, other, value)
        blocks = []
        for start in range(0, value.shape[1], width):
            blocks += [first[:, start : start + width], second[:, start : start + width]]
        value = jnp.concatenate(blocks, axis=1)
        bit //= 2
    return value


def on_device(subj, slab, fod, rotation, modulation, subject_ids, subject_weight, voxel_cell_index):
    total_subjects = subject_weight.shape[0]
    coef = fod.shape[1]
    picked = subject_ids[:, None] == jnp.arange(total_subjects, dtype=jnp.int32)[None, :]
    weight = modulation * jnp.sum(jnp.where(picked, subject_weight[None, :], 0.0), axis=1)[:, None]
    weighted_fod = fod.astype(jnp.float32) * weight[:, None, :]
    numer = jnp.sum(rotation.astype(jnp.float32) * weighted_fod[:, None], axis=(0, 2))
    sums = jnp.concatenate([numer, jnp.sum(weight, axis=0)[None]], axis=0)
    sums = butterfly_sum(sums, "subj", subj)
    average = (sums[:coef] / sums[coef:]).astype(jnp.bfloat16)
    onehot = (voxel_cell_index[:, None] == jnp.arange(GRID_DEV, dtype=jnp.int32)[None, :]).astype(jnp.bfloat16)
    dense = jnp.dot(average, onehot, preferred_element_type=jnp.float32).astype(jnp.bfloat16)
    return butterfly_gather(dense, "slab", slab)


def solution(mesh):
    placed = (
        P("subj", None, "slab"),
        P("subj", None, None, "slab"),
        P("subj", "slab"),
        P("subj"),
        P(),
        P("slab"),
    )
    subj, slab = mesh.shape["subj"], mesh.shape["slab"]

    def body(*args):
        return on_device(subj, slab, *args)

    return jax.shard_map(body, mesh=mesh, in_specs=placed, out_specs=P(), check_vma=False)
```

```python
import functools

import jax
import jax.numpy as jnp
from jax import lax
from jax.experimental import pallas as pl
from jax.experimental.pallas import tpu as pltpu
from jax.sharding import PartitionSpec as P

GRID_DEV = 1024
LANES = 128


def exchange(value, axis, size, bit):
    return lax.ppermute(value, axis, [(i, i ^ bit) for i in range(size)])


def butterfly_sum(value, axis, size):
    if size & (size - 1):
        return lax.psum(value, axis)
    bit = 1
    while bit < size:
        value = value + exchange(value, axis, size, bit)
        bit *= 2
    return value


def butterfly_gather(value, axis, size):
    if size & (size - 1):
        return lax.all_gather(value, axis, axis=1, tiled=True)
    index = lax.axis_index(axis)
    width = value.shape[1]
    bit = size // 2
    while bit:
        other = exchange(value, axis, size, bit)
        low = (index & bit) == 0
        first, second = jnp.where(low, value, other), jnp.where(low, other, value)
        blocks = []
        for start in range(0, value.shape[1], width):
            blocks += [first[:, start : start + width], second[:, start : start + width]]
        value = jnp.concatenate(blocks, axis=1)
        bit //= 2
    return value


def sums_kernel(
    subjects,
    chunk,
    rotation_hbm,
    fod_hbm,
    modulation_hbm,
    ids_hbm,
    study_hbm,
    out_ref,
    rotation,
    fod,
    modulation,
    ids,
    study,
    weighted,
    partial,
    big_sem,
    small_sem,
):
    coef, _, rows, _ = rotation.shape
    small = [
        pltpu.make_async_copy(ids_hbm, ids, small_sem.at[0]),
        pltpu.make_async_copy(study_hbm, study, small_sem.at[1]),
        pltpu.make_async_copy(modulation_hbm, modulation, small_sem.at[2]),
        pltpu.make_async_copy(fod_hbm, fod, small_sem.at[3]),
    ]
    for copy in small:
        copy.start()

    def big(step):
        part = pl.ds(step * chunk, chunk)
        return pltpu.make_async_copy(rotation_hbm.at[part], rotation.at[part], big_sem.at[step])

    for step in range(coef // chunk):
        big(step).start()
    for copy in small:
        copy.wait()

    subject = lax.broadcasted_iota(jnp.int32, (rows, LANES), 0) % subjects
    factor = jnp.zeros((rows, LANES), jnp.float32)
    for s in range(subjects):
        factor = jnp.where(subject == s, study[ids[s]], factor)
    weight = modulation[...] * factor
    partial[pl.ds(coef * rows, rows)] = weight
    for k in range(coef):
        weighted[k] = fod[k].astype(jnp.float32) * weight

    @pl.loop(0, coef // chunk)
    def _(step):
        big(step).wait()
        total = [jnp.zeros((rows, LANES), jnp.float32) for _ in range(chunk)]
        for k in range(coef):
            term = weighted[k]
            for c in range(chunk):
                total[c] += rotation[step * chunk + c, k].astype(jnp.float32) * term
        for c in range(chunk):
            partial[pl.ds(pl.multiple_of((step * chunk + c) * rows, rows), rows)] = total[c]

    count = out_ref.shape[0]
    out = partial[pl.ds(0, count, stride=subjects)]
    for s in range(1, subjects):
        out += partial[pl.ds(s, count, stride=subjects)]
    out_ref[...] = out


def local_sums(fod, rotation, modulation, subject_ids, subject_weight):
    subjects, coef, voxels = fod.shape
    blocks = voxels // LANES
    rows = blocks * subjects
    chunk = next(n for n in (5, 4, 3, 2, 1) if coef % n == 0)
    turned = rotation.transpose(1, 2, 0, 3).reshape(coef, coef, subjects, blocks, LANES)
    turned = turned.transpose(0, 1, 3, 2, 4).reshape(coef, coef, rows, LANES)
    fod = fod.transpose(1, 0, 2).reshape(coef, subjects, blocks, LANES).transpose(0, 2, 1, 3).reshape(coef, rows, LANES)
    modulation = modulation.reshape(subjects, blocks, LANES).transpose(1, 0, 2).reshape(rows, LANES)
    return pl.pallas_call(
        functools.partial(sums_kernel, subjects, chunk),
        out_shape=jax.ShapeDtypeStruct(((coef + 1) * blocks, LANES), jnp.float32),
        in_specs=[pl.BlockSpec(memory_space=pl.ANY)] * 5,
        out_specs=pl.BlockSpec(memory_space=pltpu.VMEM),
        scratch_shapes=[
            pltpu.VMEM(turned.shape, turned.dtype),
            pltpu.VMEM(fod.shape, fod.dtype),
            pltpu.VMEM(modulation.shape, jnp.float32),
            pltpu.SMEM(subject_ids.shape, jnp.int32),
            pltpu.SMEM(subject_weight.shape, jnp.float32),
            pltpu.VMEM(fod.shape, jnp.float32),
            pltpu.VMEM(((coef + 1) * rows, LANES), jnp.float32),
            pltpu.SemaphoreType.DMA((coef // chunk,)),
            pltpu.SemaphoreType.DMA((4,)),
        ],
        name="local_sums",
    )(turned, fod, modulation, subject_ids, subject_weight)


def on_device(subj, slab, fod, rotation, modulation, subject_ids, subject_weight, voxel_cell_index):
    coef, voxels = fod.shape[1:]
    sums = local_sums(fod, rotation, modulation, subject_ids, subject_weight)
    sums = butterfly_sum(sums, "subj", subj).reshape(coef + 1, voxels)
    average = (sums[:coef] / sums[coef:]).astype(jnp.bfloat16)
    onehot = (voxel_cell_index[:, None] == jnp.arange(GRID_DEV, dtype=jnp.int32)[None, :]).astype(jnp.bfloat16)
    dense = jnp.dot(average, onehot, preferred_element_type=jnp.float32).astype(jnp.bfloat16)
    return butterfly_gather(dense, "slab", slab)


def solution(mesh):
    placed = (
        P("subj", None, "slab"),
        P("subj", None, None, "slab"),
        P("subj", "slab"),
        P("subj"),
        P(),
        P("slab"),
    )
    subj, slab = mesh.shape["subj"], mesh.shape["slab"]

    def body(*args):
        return on_device(subj, slab, *args)

    return jax.shard_map(body, mesh=mesh, in_specs=placed, out_specs=P(), check_vma=False)
```

```python
import functools

import jax
import jax.numpy as jnp
from jax import lax
from jax.experimental import pallas as pl
from jax.experimental.pallas import tpu as pltpu
from jax.sharding import PartitionSpec as P

GRID_DEV = 1024
LANES = 128


def exchange(value, axis, size, bit):
    return lax.ppermute(value, axis, [(i, i ^ bit) for i in range(size)])


def butterfly_sum(value, axis, size):
    if size & (size - 1):
        return lax.psum(value, axis)
    bit = 1
    while bit < size:
        value = value + exchange(value, axis, size, bit)
        bit *= 2
    return value


def butterfly_gather(value, axis, size):
    if size & (size - 1):
        return lax.all_gather(value, axis, axis=1, tiled=True)
    index = lax.axis_index(axis)
    width = value.shape[1]
    bit = size // 2
    while bit:
        other = exchange(value, axis, size, bit)
        low = (index & bit) == 0
        first, second = jnp.where(low, value, other), jnp.where(low, other, value)
        blocks = []
        for start in range(0, value.shape[1], width):
            blocks += [first[:, start : start + width], second[:, start : start + width]]
        value = jnp.concatenate(blocks, axis=1)
        bit //= 2
    return value


def sums_kernel(
    subjects,
    chunk,
    rotation_hbm,
    fod_hbm,
    modulation_hbm,
    ids_hbm,
    study_hbm,
    out_ref,
    rotation,
    fod,
    modulation,
    ids,
    study,
    weighted,
    partial,
    big_sem,
    small_sem,
):
    coef, _, rows, _ = rotation.shape
    small = [
        pltpu.make_async_copy(ids_hbm, ids, small_sem.at[0]),
        pltpu.make_async_copy(study_hbm, study, small_sem.at[1]),
        pltpu.make_async_copy(modulation_hbm, modulation, small_sem.at[2]),
        pltpu.make_async_copy(fod_hbm, fod, small_sem.at[3]),
    ]
    for copy in small:
        copy.start()

    def big(step):
        part = pl.ds(step * chunk, chunk)
        return pltpu.make_async_copy(rotation_hbm.at[part], rotation.at[part], big_sem.at[step])

    for step in range(coef // chunk):
        big(step).start(priority=1)
    for copy in small:
        copy.wait()

    subject = lax.broadcasted_iota(jnp.int32, (rows, LANES), 0) % subjects
    factor = jnp.zeros((rows, LANES), jnp.float32)
    for s in range(subjects):
        factor = jnp.where(subject == s, study[ids[s]], factor)
    weight = modulation[...] * factor
    partial[pl.ds(coef * rows, rows)] = weight
    for k in range(coef):
        weighted[k] = fod[k].astype(jnp.float32) * weight

    @pl.loop(0, coef // chunk)
    def _(step):
        big(step).wait()
        total = [jnp.zeros((rows, LANES), jnp.float32) for _ in range(chunk)]
        for k in range(coef):
            term = weighted[k]
            for c in range(chunk):
                total[c] += rotation[step * chunk + c, k].astype(jnp.float32) * term
        for c in range(chunk):
            partial[pl.ds(pl.multiple_of((step * chunk + c) * rows, rows), rows)] = total[c]

    count = out_ref.shape[0]
    out = partial[pl.ds(0, count, stride=subjects)]
    for s in range(1, subjects):
        out += partial[pl.ds(s, count, stride=subjects)]
    out_ref[...] = out


def local_sums(fod, rotation, modulation, subject_ids, subject_weight):
    subjects, coef, voxels = fod.shape
    blocks = voxels // LANES
    rows = blocks * subjects
    chunk = next(n for n in (5, 4, 3, 2, 1) if coef % n == 0)
    turned = rotation.transpose(1, 2, 0, 3).reshape(coef, coef, subjects, blocks, LANES)
    turned = turned.transpose(0, 1, 3, 2, 4).reshape(coef, coef, rows, LANES)
    fod = fod.transpose(1, 0, 2).reshape(coef, subjects, blocks, LANES).transpose(0, 2, 1, 3).reshape(coef, rows, LANES)
    modulation = modulation.reshape(subjects, blocks, LANES).transpose(1, 0, 2).reshape(rows, LANES)
    return pl.pallas_call(
        functools.partial(sums_kernel, subjects, chunk),
        out_shape=pltpu.VMEM(((coef + 1) * blocks, LANES), jnp.float32),
        in_specs=[pl.BlockSpec(memory_space=pl.ANY)] * 5,
        out_specs=pl.BlockSpec(memory_space=pltpu.VMEM),
        scratch_shapes=[
            pltpu.VMEM(turned.shape, turned.dtype),
            pltpu.VMEM(fod.shape, fod.dtype),
            pltpu.VMEM(modulation.shape, jnp.float32),
            pltpu.SMEM(subject_ids.shape, jnp.int32),
            pltpu.SMEM(subject_weight.shape, jnp.float32),
            pltpu.VMEM(fod.shape, jnp.float32),
            pltpu.VMEM(((coef + 1) * rows, LANES), jnp.float32),
            pltpu.SemaphoreType.DMA((coef // chunk,)),
            pltpu.SemaphoreType.DMA((4,)),
        ],
        compiler_params=pltpu.CompilerParams(vmem_limit_bytes=32 << 20),
        name="local_sums",
    )(*[pltpu.with_memory_space_constraint(x, pltpu.HBM) for x in (turned, fod, modulation, subject_ids, subject_weight)])


def on_device(subj, slab, fod, rotation, modulation, subject_ids, subject_weight, voxel_cell_index):
    coef, voxels = fod.shape[1:]
    sums = local_sums(fod, rotation, modulation, subject_ids, subject_weight)
    sums = butterfly_sum(sums, "subj", subj).reshape(coef + 1, voxels)
    average = (sums[:coef] / sums[coef:]).astype(jnp.bfloat16)
    onehot = (voxel_cell_index[:, None] == jnp.arange(GRID_DEV, dtype=jnp.int32)[None, :]).astype(jnp.bfloat16)
    dense = jnp.dot(average, onehot, preferred_element_type=jnp.float32).astype(jnp.bfloat16)
    return butterfly_gather(dense, "slab", slab)


def solution(mesh):
    placed = (
        P("subj", None, "slab"),
        P("subj", None, None, "slab"),
        P("subj", "slab"),
        P("subj"),
        P(),
        P("slab"),
    )
    subj, slab = mesh.shape["subj"], mesh.shape["slab"]

    def body(*args):
        return on_device(subj, slab, *args)

    return jax.shard_map(body, mesh=mesh, in_specs=placed, out_specs=P(), check_vma=False)
```

```python
import functools

import jax
import jax.numpy as jnp
from jax import lax
from jax.experimental import pallas as pl
from jax.experimental.pallas import tpu as pltpu
from jax.sharding import PartitionSpec as P

GRID_DEV = 1024
LANES = 128
SPLIT = 32


def exchange(value, axis, size, bit):
    return lax.ppermute(value, axis, [(i, i ^ bit) for i in range(size)])


def sums_kernel(
    subjects,
    chunk,
    rotation_hbm,
    fod_hbm,
    modulation_hbm,
    ids_hbm,
    study_hbm,
    out_ref,
    rotation,
    fod,
    modulation,
    ids,
    study,
    weighted,
    partial,
    big_sem,
    small_sem,
):
    coef, _, rows, _ = rotation.shape
    small = [
        pltpu.make_async_copy(ids_hbm, ids, small_sem.at[0]),
        pltpu.make_async_copy(study_hbm, study, small_sem.at[1]),
        pltpu.make_async_copy(modulation_hbm, modulation, small_sem.at[2]),
        pltpu.make_async_copy(fod_hbm, fod, small_sem.at[3]),
    ]
    for copy in small:
        copy.start()

    def big(step):
        part = pl.ds(step * chunk, chunk)
        return pltpu.make_async_copy(rotation_hbm.at[part], rotation.at[part], big_sem.at[step])

    for step in range(coef // chunk):
        big(step).start(priority=1)
    for copy in small:
        copy.wait()

    subject = lax.broadcasted_iota(jnp.int32, (rows, LANES), 0) % subjects
    factor = jnp.zeros((rows, LANES), jnp.float32)
    for s in range(subjects):
        factor = jnp.where(subject == s, study[ids[s]], factor)
    weight = modulation[...] * factor
    partial[pl.ds(coef * rows, rows)] = weight
    for k in range(coef):
        weighted[k] = fod[k].astype(jnp.float32) * weight

    @pl.loop(0, coef // chunk)
    def _(step):
        big(step).wait()
        total = [jnp.zeros((rows, LANES), jnp.float32) for _ in range(chunk)]
        for k in range(coef):
            term = weighted[k]
            for c in range(chunk):
                total[c] += rotation[step * chunk + c, k].astype(jnp.float32) * term
        for c in range(chunk):
            partial[pl.ds(pl.multiple_of((step * chunk + c) * rows, rows), rows)] = total[c]

    count = out_ref.shape[0]
    out = partial[pl.ds(0, count, stride=subjects)]
    for s in range(1, subjects):
        out += partial[pl.ds(s, count, stride=subjects)]
    out_ref[...] = out


def local_sums(fod, rotation, modulation, subject_ids, subject_weight):
    subjects, coef, voxels = fod.shape
    blocks = voxels // LANES
    rows = blocks * subjects
    chunk = next(n for n in (5, 4, 3, 2, 1) if coef % n == 0)
    turned = rotation.transpose(1, 2, 0, 3).reshape(coef, coef, subjects, blocks, LANES)
    turned = turned.transpose(0, 1, 3, 2, 4).reshape(coef, coef, rows, LANES)
    fod = fod.transpose(1, 0, 2).reshape(coef, subjects, blocks, LANES).transpose(0, 2, 1, 3).reshape(coef, rows, LANES)
    modulation = modulation.reshape(subjects, blocks, LANES).transpose(1, 0, 2).reshape(rows, LANES)
    return pl.pallas_call(
        functools.partial(sums_kernel, subjects, chunk),
        out_shape=pltpu.VMEM(((coef + 1) * blocks, LANES), jnp.float32),
        in_specs=[pl.BlockSpec(memory_space=pl.ANY)] * 5,
        out_specs=pl.BlockSpec(memory_space=pltpu.VMEM),
        scratch_shapes=[
            pltpu.VMEM(turned.shape, turned.dtype),
            pltpu.VMEM(fod.shape, fod.dtype),
            pltpu.VMEM(modulation.shape, jnp.float32),
            pltpu.SMEM(subject_ids.shape, jnp.int32),
            pltpu.SMEM(subject_weight.shape, jnp.float32),
            pltpu.VMEM(fod.shape, jnp.float32),
            pltpu.VMEM(((coef + 1) * rows, LANES), jnp.float32),
            pltpu.SemaphoreType.DMA((coef // chunk,)),
            pltpu.SemaphoreType.DMA((4,)),
        ],
        compiler_params=pltpu.CompilerParams(vmem_limit_bytes=32 << 20),
        name="local_sums",
    )(*[pltpu.with_memory_space_constraint(x, pltpu.HBM) for x in (turned, fod, modulation, subject_ids, subject_weight)])


def finish_kernel(coef, mine_ref, other_ref, cells_ref, out_ref, total):
    rows, voxels = out_ref.shape
    blocks = voxels // LANES
    total[pl.ds(0, mine_ref.shape[0])] = mine_ref[...] + other_ref[...]
    row = lax.broadcasted_iota(jnp.int32, (rows, LANES), 0)
    for block in range(blocks):
        numer = total[pl.ds(block, rows, stride=blocks)]
        denom = total[pl.ds(coef * blocks + block, 1)]
        cells = cells_ref[pl.ds(block, 1)]
        high, low = (cells // SPLIT).astype(jnp.float32), (cells % SPLIT).astype(jnp.float32)
        value = jnp.where(row < coef, numer / denom, jnp.where(row == coef, high, jnp.where(row == coef + 1, low, 0.0)))
        out_ref[:, pl.ds(block * LANES, LANES)] = value.astype(jnp.bfloat16)


def finish(mine, other, cells, coef):
    blocks = cells.shape[0] // LANES
    rows = -(-(coef + 2) // 8) * 8
    return pl.pallas_call(
        functools.partial(finish_kernel, coef),
        out_shape=pltpu.VMEM((rows, cells.shape[0]), jnp.bfloat16),
        in_specs=[pl.BlockSpec(memory_space=pltpu.VMEM)] * 3,
        out_specs=pl.BlockSpec(memory_space=pltpu.VMEM),
        scratch_shapes=[pltpu.VMEM((rows * blocks, LANES), jnp.float32)],
        compiler_params=pltpu.CompilerParams(vmem_limit_bytes=16 << 20),
        name="finish",
    )(mine, other, cells.reshape(blocks, LANES))


def dense_of(coef, compact):
    voxels = compact.shape[1]
    high = compact[coef : coef + 1].astype(jnp.float32)
    low = compact[coef + 1 : coef + 2].astype(jnp.float32)
    cells = (high * SPLIT + low).astype(jnp.int32)
    hit = lax.broadcasted_iota(jnp.int32, (GRID_DEV, voxels), 0) == cells
    onehot = jnp.where(hit, 1.0, 0.0).astype(jnp.bfloat16)
    dense = lax.dot_general(compact, onehot, (((1,), (1,)), ((), ())), preferred_element_type=jnp.float32)
    return dense[:coef].astype(jnp.bfloat16)


def place_first_kernel(coef, compact_ref, out_ref):
    out_ref[...] = dense_of(coef, compact_ref[...])


def place_next_kernel(coef, first_ref, compact_ref, out_ref):
    width = first_ref.shape[1]
    out_ref[:, pl.ds(0, width)] = first_ref[...]
    out_ref[:, pl.ds(width, GRID_DEV)] = dense_of(coef, compact_ref[...])


def place(coef, first, compact):
    operands = (compact,) if first is None else (first, compact)
    width = GRID_DEV if first is None else first.shape[1] + GRID_DEV
    return pl.pallas_call(
        functools.partial(place_first_kernel if first is None else place_next_kernel, coef),
        out_shape=pltpu.VMEM((coef, width), jnp.bfloat16),
        in_specs=[pl.BlockSpec(memory_space=pltpu.VMEM)] * len(operands),
        out_specs=pl.BlockSpec(memory_space=pltpu.VMEM),
        cost_estimate=pl.CostEstimate(flops=2 * coef * compact.shape[1] * GRID_DEV, bytes_accessed=1 << 18, transcendentals=0),
        compiler_params=pltpu.CompilerParams(vmem_limit_bytes=32 << 20),
        name="place",
    )(*operands)


def on_device(subj, slab, fod, rotation, modulation, subject_ids, subject_weight, voxel_cell_index):
    coef = fod.shape[1]
    mine = local_sums(fod, rotation, modulation, subject_ids, subject_weight)
    bit = 1
    while 2 * bit < subj:
        mine = mine + exchange(mine, "subj", subj, bit)
        bit *= 2
    compact = finish(mine, exchange(mine, "subj", subj, bit), voxel_cell_index, coef)
    bits = [1 << n for n in reversed(range(slab.bit_length() - 1))]
    other = exchange(compact, "slab", slab, bits[0])
    dense = place(coef, place(coef, None, compact), other)
    order = [0, bits[0]]
    for bit in bits[1:]:
        dense = jnp.concatenate([dense, exchange(dense, "slab", slab, bit)], axis=1)
        order += [o ^ bit for o in order]
    index = lax.axis_index("slab")
    blocks = {o: dense[:, i * GRID_DEV : (i + 1) * GRID_DEV] for i, o in enumerate(order)}
    for bit in bits:
        flip = (index & bit) != 0
        blocks = {o: jnp.where(flip, blocks[o ^ bit], blocks[o]) for o in blocks}
    return jnp.concatenate([blocks[o] for o in range(slab)], axis=1)


def solution(mesh):
    placed = (
        P("subj", None, "slab"),
        P("subj", None, None, "slab"),
        P("subj", "slab"),
        P("subj"),
        P(),
        P("slab"),
    )
    subj, slab = mesh.shape["subj"], mesh.shape["slab"]

    def body(*args):
        return on_device(subj, slab, *args)

    return jax.shard_map(body, mesh=mesh, in_specs=placed, out_specs=P(), check_vma=False)
```

```python
import functools

import jax
import jax.numpy as jnp
from jax import lax
from jax.experimental import pallas as pl
from jax.experimental.pallas import tpu as pltpu
from jax.sharding import PartitionSpec as P

GRID_DEV = 1024
LANES = 128
SPLIT = 32
TILE = 256


def exchange(value, axis, size, bit):
    return lax.ppermute(value, axis, [(i, i ^ bit) for i in range(size)])


def sums_kernel(
    subjects,
    chunk,
    rotation_hbm,
    fod_hbm,
    modulation_hbm,
    ids_hbm,
    study_hbm,
    out_ref,
    rotation,
    fod,
    modulation,
    ids,
    study,
    weighted,
    partial,
    big_sem,
    small_sem,
):
    coef, _, rows, _ = rotation.shape
    small = [
        pltpu.make_async_copy(ids_hbm, ids, small_sem.at[0]),
        pltpu.make_async_copy(study_hbm, study, small_sem.at[1]),
        pltpu.make_async_copy(modulation_hbm, modulation, small_sem.at[2]),
        pltpu.make_async_copy(fod_hbm, fod, small_sem.at[3]),
    ]
    for copy in small:
        copy.start()

    def big(step):
        part = pl.ds(step * chunk, chunk)
        return pltpu.make_async_copy(rotation_hbm.at[part], rotation.at[part], big_sem.at[step])

    for step in range(coef // chunk):
        big(step).start(priority=1)
    for copy in small:
        copy.wait()

    subject = lax.broadcasted_iota(jnp.int32, (rows, LANES), 0) % subjects
    factor = jnp.zeros((rows, LANES), jnp.float32)
    for s in range(subjects):
        factor = jnp.where(subject == s, study[ids[s]], factor)
    weight = modulation[...] * factor
    partial[pl.ds(coef * rows, rows)] = weight
    for k in range(coef):
        weighted[k] = fod[k].astype(jnp.float32) * weight

    @pl.loop(0, coef // chunk)
    def _(step):
        big(step).wait()
        total = [jnp.zeros((rows, LANES), jnp.float32) for _ in range(chunk)]
        for k in range(coef):
            term = weighted[k]
            for c in range(chunk):
                total[c] += rotation[step * chunk + c, k].astype(jnp.float32) * term
        for c in range(chunk):
            partial[pl.ds(pl.multiple_of((step * chunk + c) * rows, rows), rows)] = total[c]

    count = out_ref.shape[0]
    out = partial[pl.ds(0, count, stride=subjects)]
    for s in range(1, subjects):
        out += partial[pl.ds(s, count, stride=subjects)]
    out_ref[...] = out


def local_sums(fod, rotation, modulation, subject_ids, subject_weight):
    subjects, coef, voxels = fod.shape
    blocks = voxels // LANES
    rows = blocks * subjects
    chunk = next(n for n in (5, 4, 3, 2, 1) if coef % n == 0)
    turned = rotation.transpose(1, 2, 0, 3).reshape(coef, coef, subjects, blocks, LANES)
    turned = turned.transpose(0, 1, 3, 2, 4).reshape(coef, coef, rows, LANES)
    fod = fod.transpose(1, 0, 2).reshape(coef, subjects, blocks, LANES).transpose(0, 2, 1, 3).reshape(coef, rows, LANES)
    modulation = modulation.reshape(subjects, blocks, LANES).transpose(1, 0, 2).reshape(rows, LANES)
    return pl.pallas_call(
        functools.partial(sums_kernel, subjects, chunk),
        out_shape=pltpu.VMEM(((coef + 1) * blocks, LANES), jnp.float32),
        in_specs=[pl.BlockSpec(memory_space=pl.ANY)] * 5,
        out_specs=pl.BlockSpec(memory_space=pltpu.VMEM),
        scratch_shapes=[
            pltpu.VMEM(turned.shape, turned.dtype),
            pltpu.VMEM(fod.shape, fod.dtype),
            pltpu.VMEM(modulation.shape, jnp.float32),
            pltpu.SMEM(subject_ids.shape, jnp.int32),
            pltpu.SMEM(subject_weight.shape, jnp.float32),
            pltpu.VMEM(fod.shape, jnp.float32),
            pltpu.VMEM(((coef + 1) * rows, LANES), jnp.float32),
            pltpu.SemaphoreType.DMA((coef // chunk,)),
            pltpu.SemaphoreType.DMA((4,)),
        ],
        compiler_params=pltpu.CompilerParams(vmem_limit_bytes=32 << 20),
        name="local_sums",
    )(*[pltpu.with_memory_space_constraint(x, pltpu.HBM) for x in (turned, fod, modulation, subject_ids, subject_weight)])


def finish_kernel(coef, mine_ref, other_ref, cells_ref, out_ref, total):
    rows, voxels = out_ref.shape
    blocks = voxels // LANES
    total[pl.ds(0, mine_ref.shape[0])] = mine_ref[...] + other_ref[...]
    row = lax.broadcasted_iota(jnp.int32, (rows, LANES), 0)
    for block in range(blocks):
        numer = total[pl.ds(block, rows, stride=blocks)]
        denom = total[pl.ds(coef * blocks + block, 1)]
        cells = cells_ref[pl.ds(block, 1)]
        high, low = (cells // SPLIT).astype(jnp.float32), (cells % SPLIT).astype(jnp.float32)
        value = jnp.where(row < coef, numer / denom, jnp.where(row == coef, high, jnp.where(row == coef + 1, low, 0.0)))
        out_ref[:, pl.ds(block * LANES, LANES)] = value.astype(jnp.bfloat16)


def finish(mine, other, cells, coef):
    blocks = cells.shape[0] // LANES
    rows = -(-(coef + 2) // 8) * 8
    return pl.pallas_call(
        functools.partial(finish_kernel, coef),
        out_shape=pltpu.VMEM((rows, cells.shape[0]), jnp.bfloat16),
        in_specs=[pl.BlockSpec(memory_space=pltpu.VMEM)] * 3,
        out_specs=pl.BlockSpec(memory_space=pltpu.VMEM),
        scratch_shapes=[pltpu.VMEM((rows * blocks, LANES), jnp.float32)],
        compiler_params=pltpu.CompilerParams(vmem_limit_bytes=16 << 20),
        name="finish",
    )(mine, other, cells.reshape(blocks, LANES))


def dense_of(coef, compact):
    voxels = compact.shape[1]
    high = compact[coef : coef + 1].astype(jnp.float32)
    low = compact[coef + 1 : coef + 2].astype(jnp.float32)
    cells = (high * SPLIT + low).astype(jnp.int32)
    tiles = []
    for start in range(0, GRID_DEV, TILE):
        first = max(start - (GRID_DEV - voxels), 0) // TILE * TILE
        last = min(start + TILE, voxels)
        hit = lax.broadcasted_iota(jnp.int32, (TILE, last - first), 0) + start == cells[:, first:last]
        onehot = jnp.where(hit, 1.0, 0.0).astype(jnp.bfloat16)
        tiles.append(
            lax.dot_general(compact[:, first:last], onehot, (((1,), (1,)), ((), ())), preferred_element_type=jnp.float32)
        )
    return jnp.concatenate(tiles, axis=1)[:coef].astype(jnp.bfloat16)


def place_kernel(coef, compact_ref, out_ref):
    out_ref[...] = dense_of(coef, compact_ref[...])


def place(coef, compact):
    return pl.pallas_call(
        functools.partial(place_kernel, coef),
        out_shape=pltpu.VMEM((coef, GRID_DEV), jnp.bfloat16),
        in_specs=[pl.BlockSpec(memory_space=pltpu.VMEM)],
        out_specs=pl.BlockSpec(memory_space=pltpu.VMEM),
        cost_estimate=pl.CostEstimate(flops=2 * coef * compact.shape[1] * GRID_DEV, bytes_accessed=1 << 18, transcendentals=0),
        compiler_params=pltpu.CompilerParams(vmem_limit_bytes=32 << 20),
        name="place",
    )(compact)


def template_kernel(coef, order, *refs):
    *ready, compact_ref, out_ref, last, sem = refs
    index = lax.axis_index("slab")

    def write(i, ref):
        columns = pl.ds(pl.multiple_of((index ^ order[i]) * GRID_DEV, GRID_DEV), GRID_DEV)
        return pltpu.make_async_copy(ref, out_ref.at[:, columns], sem.at[i])

    copies = [write(i, ref) for i, ref in enumerate(ready)]
    for copy in copies:
        copy.start()
    last[...] = dense_of(coef, compact_ref[...])
    copies.append(write(len(ready), last))
    copies[-1].start()
    for copy in copies:
        copy.wait()


def template(coef, order, ready, compact):
    return pl.pallas_call(
        functools.partial(template_kernel, coef, order),
        out_shape=jax.ShapeDtypeStruct((coef, len(order) * GRID_DEV), jnp.bfloat16),
        in_specs=[pl.BlockSpec(memory_space=pltpu.VMEM)] * len(order),
        out_specs=pl.BlockSpec(memory_space=pl.ANY),
        scratch_shapes=[pltpu.VMEM((coef, GRID_DEV), jnp.bfloat16), pltpu.SemaphoreType.DMA((len(order),))],
        compiler_params=pltpu.CompilerParams(vmem_limit_bytes=32 << 20),
        name="template",
    )(*ready, compact)


def on_device(subj, slab, fod, rotation, modulation, subject_ids, subject_weight, voxel_cell_index):
    coef = fod.shape[1]
    mine = local_sums(fod, rotation, modulation, subject_ids, subject_weight)
    bit = 1
    while 2 * bit < subj:
        mine = mine + exchange(mine, "subj", subj, bit)
        bit *= 2
    pieces = {0: finish(mine, exchange(mine, "subj", subj, bit), voxel_cell_index, coef)}
    pieces[1] = exchange(pieces[0], "slab", slab, 1)
    dense = {o: place(coef, piece) for o, piece in pieces.items()}
    bit = slab // 2
    while bit > 1:
        for o in [o for o in pieces if not o & 1]:
            far = o ^ bit
            pieces[far] = exchange(pieces[o], "slab", slab, bit)
            dense, pieces[far] = lax.optimization_barrier((dense, pieces[far]))
            pieces[far ^ 1] = exchange(pieces[far], "slab", slab, 1)
            dense[far] = place(coef, pieces[far])
            if len(pieces) < slab:
                dense[far ^ 1] = place(coef, pieces[far ^ 1])
        bit //= 2
    return template(coef, (*dense, last := list(pieces)[-1]), list(dense.values()), pieces[last])


def solution(mesh):
    placed = (
        P("subj", None, "slab"),
        P("subj", None, None, "slab"),
        P("subj", "slab"),
        P("subj"),
        P(),
        P("slab"),
    )
    subj, slab = mesh.shape["subj"], mesh.shape["slab"]

    def body(*args):
        return on_device(subj, slab, *args)

    return jax.shard_map(body, mesh=mesh, in_specs=placed, out_specs=P(), check_vma=False)
```

```python
import functools

import jax
import jax.numpy as jnp
from jax import lax
from jax.experimental import pallas as pl
from jax.experimental.pallas import tpu as pltpu
from jax.sharding import PartitionSpec as P

GRID_DEV = 1024
LANES = 128
SPLIT = 32
TILE = 256


def exchange(value, axis, size, bit):
    return lax.ppermute(value, axis, [(i, i ^ bit) for i in range(size)])


def sums_kernel(
    subjects,
    chunk,
    rotation_hbm,
    fod_hbm,
    modulation_hbm,
    ids_hbm,
    study_hbm,
    out_ref,
    rotation,
    fod,
    modulation,
    ids,
    study,
    weighted,
    partial,
    big_sem,
    small_sem,
):
    coef, _, rows, _ = rotation.shape
    small = [
        pltpu.make_async_copy(ids_hbm, ids, small_sem.at[0]),
        pltpu.make_async_copy(study_hbm, study, small_sem.at[1]),
        pltpu.make_async_copy(modulation_hbm, modulation, small_sem.at[2]),
        pltpu.make_async_copy(fod_hbm, fod, small_sem.at[3]),
    ]
    for copy in small:
        copy.start()

    def big(step):
        part = pl.ds(step * chunk, chunk)
        return pltpu.make_async_copy(rotation_hbm.at[part], rotation.at[part], big_sem.at[step])

    for step in range(coef // chunk):
        big(step).start(priority=1)
    for copy in small:
        copy.wait()

    subject = lax.broadcasted_iota(jnp.int32, (rows, LANES), 0) % subjects
    factor = jnp.zeros((rows, LANES), jnp.float32)
    for s in range(subjects):
        factor = jnp.where(subject == s, study[ids[s]], factor)
    weight = modulation[...] * factor
    partial[pl.ds(coef * rows, rows)] = weight
    for k in range(coef):
        weighted[k] = fod[k].astype(jnp.float32) * weight

    @pl.loop(0, coef // chunk)
    def _(step):
        big(step).wait()
        total = [jnp.zeros((rows, LANES), jnp.float32) for _ in range(chunk)]
        for k in range(coef):
            term = weighted[k]
            for c in range(chunk):
                total[c] += rotation[step * chunk + c, k].astype(jnp.float32) * term
        for c in range(chunk):
            partial[pl.ds(pl.multiple_of((step * chunk + c) * rows, rows), rows)] = total[c]

    count = out_ref.shape[0]
    out = partial[pl.ds(0, count, stride=subjects)]
    for s in range(1, subjects):
        out += partial[pl.ds(s, count, stride=subjects)]
    out_ref[...] = out


def local_sums(fod, rotation, modulation, subject_ids, subject_weight):
    subjects, coef, voxels = fod.shape
    blocks = voxels // LANES
    rows = blocks * subjects
    chunk = next(n for n in (5, 4, 3, 2, 1) if coef % n == 0)
    turned = rotation.transpose(1, 2, 0, 3).reshape(coef, coef, subjects, blocks, LANES)
    turned = turned.transpose(0, 1, 3, 2, 4).reshape(coef, coef, rows, LANES)
    fod = fod.transpose(1, 0, 2).reshape(coef, subjects, blocks, LANES).transpose(0, 2, 1, 3).reshape(coef, rows, LANES)
    modulation = modulation.reshape(subjects, blocks, LANES).transpose(1, 0, 2).reshape(rows, LANES)
    return pl.pallas_call(
        functools.partial(sums_kernel, subjects, chunk),
        out_shape=pltpu.VMEM(((coef + 1) * blocks, LANES), jnp.float32),
        in_specs=[pl.BlockSpec(memory_space=pl.ANY)] * 5,
        out_specs=pl.BlockSpec(memory_space=pltpu.VMEM),
        scratch_shapes=[
            pltpu.VMEM(turned.shape, turned.dtype),
            pltpu.VMEM(fod.shape, fod.dtype),
            pltpu.VMEM(modulation.shape, jnp.float32),
            pltpu.SMEM(subject_ids.shape, jnp.int32),
            pltpu.SMEM(subject_weight.shape, jnp.float32),
            pltpu.VMEM(fod.shape, jnp.float32),
            pltpu.VMEM(((coef + 1) * rows, LANES), jnp.float32),
            pltpu.SemaphoreType.DMA((coef // chunk,)),
            pltpu.SemaphoreType.DMA((4,)),
        ],
        compiler_params=pltpu.CompilerParams(vmem_limit_bytes=32 << 20),
        name="local_sums",
    )(*[pltpu.with_memory_space_constraint(x, pltpu.HBM) for x in (turned, fod, modulation, subject_ids, subject_weight)])


def finish_kernel(coef, mine_ref, other_ref, cells_ref, out_ref, total):
    rows, voxels = out_ref.shape
    blocks = voxels // LANES
    total[pl.ds(0, mine_ref.shape[0])] = mine_ref[...] + other_ref[...]
    row = lax.broadcasted_iota(jnp.int32, (rows, LANES), 0)
    for block in range(blocks):
        numer = total[pl.ds(block, rows, stride=blocks)]
        denom = total[pl.ds(coef * blocks + block, 1)]
        cells = cells_ref[pl.ds(block, 1)]
        high, low = (cells // SPLIT).astype(jnp.float32), (cells % SPLIT).astype(jnp.float32)
        value = jnp.where(row < coef, numer / denom, jnp.where(row == coef, high, jnp.where(row == coef + 1, low, 0.0)))
        out_ref[:, pl.ds(block * LANES, LANES)] = value.astype(jnp.bfloat16)


def finish(mine, other, cells, coef):
    blocks = cells.shape[0] // LANES
    rows = -(-(coef + 2) // 8) * 8
    return pl.pallas_call(
        functools.partial(finish_kernel, coef),
        out_shape=pltpu.VMEM((rows, cells.shape[0]), jnp.bfloat16),
        in_specs=[pl.BlockSpec(memory_space=pltpu.VMEM)] * 3,
        out_specs=pl.BlockSpec(memory_space=pltpu.VMEM),
        scratch_shapes=[pltpu.VMEM((rows * blocks, LANES), jnp.float32)],
        compiler_params=pltpu.CompilerParams(vmem_limit_bytes=16 << 20),
        name="finish",
    )(mine, other, cells.reshape(blocks, LANES))


def dense_of(coef, compact):
    voxels = compact.shape[1]
    high = compact[coef : coef + 1].astype(jnp.float32)
    low = compact[coef + 1 : coef + 2].astype(jnp.float32)
    cells = (high * SPLIT + low).astype(jnp.int32)
    tiles = []
    for start in range(0, GRID_DEV, TILE):
        first = max(start - (GRID_DEV - voxels), 0) // TILE * TILE
        last = min(start + TILE, voxels)
        hit = lax.broadcasted_iota(jnp.int32, (TILE, last - first), 0) + start == cells[:, first:last]
        onehot = jnp.where(hit, 1.0, 0.0).astype(jnp.bfloat16)
        tiles.append(
            lax.dot_general(compact[:, first:last], onehot, (((1,), (1,)), ((), ())), preferred_element_type=jnp.float32)
        )
    return jnp.concatenate(tiles, axis=1)[:coef].astype(jnp.bfloat16)


def place_kernel(coef, compact_ref, out_ref):
    out_ref[...] = dense_of(coef, compact_ref[...])


def place(coef, compact):
    return pl.pallas_call(
        functools.partial(place_kernel, coef),
        out_shape=pltpu.VMEM((coef, GRID_DEV), jnp.bfloat16),
        in_specs=[pl.BlockSpec(memory_space=pltpu.VMEM)],
        out_specs=pl.BlockSpec(memory_space=pltpu.VMEM),
        cost_estimate=pl.CostEstimate(flops=2 * coef * compact.shape[1] * GRID_DEV, bytes_accessed=1 << 18, transcendentals=0),
        compiler_params=pltpu.CompilerParams(vmem_limit_bytes=32 << 20),
        name="place",
    )(compact)


def template_kernel(coef, order, *refs):
    *ready, compact_ref, out_ref, last, sem = refs
    index = lax.axis_index("slab")

    def write(i, ref):
        columns = pl.ds(pl.multiple_of((index ^ order[i]) * GRID_DEV, GRID_DEV), GRID_DEV)
        return pltpu.make_async_copy(ref, out_ref.at[:, columns], sem.at[i])

    copies = [write(i, ref) for i, ref in enumerate(ready)]
    for copy in copies:
        copy.start()
    last[...] = dense_of(coef, compact_ref[...])
    copies.append(write(len(ready), last))
    copies[-1].start()
    for copy in copies:
        copy.wait()


def template(coef, order, ready, compact):
    return pl.pallas_call(
        functools.partial(template_kernel, coef, order),
        out_shape=jax.ShapeDtypeStruct((coef, len(order) * GRID_DEV), jnp.bfloat16),
        in_specs=[pl.BlockSpec(memory_space=pltpu.VMEM)] * len(order),
        out_specs=pl.BlockSpec(memory_space=pl.ANY),
        scratch_shapes=[pltpu.VMEM((coef, GRID_DEV), jnp.bfloat16), pltpu.SemaphoreType.DMA((len(order),))],
        compiler_params=pltpu.CompilerParams(vmem_limit_bytes=32 << 20),
        name="template",
    )(*ready, compact)


def on_device(subj, slab, fod, rotation, modulation, subject_ids, subject_weight, voxel_cell_index):
    coef = fod.shape[1]
    mine = local_sums(fod, rotation, modulation, subject_ids, subject_weight)
    bit = 1
    while 2 * bit < subj:
        mine = mine + exchange(mine, "subj", subj, bit)
        bit *= 2
    pieces = {0: finish(mine, exchange(mine, "subj", subj, bit), voxel_cell_index, coef)}
    own = pieces[0]
    for offset in reversed(range(1, slab)):
        pieces[offset] = exchange(own, "slab", slab, offset)
    last = slab // 2
    order = [o for o in sorted(pieces) if o != last] + [last]
    dense = []
    for offset in order[:-1]:
        dense.append(place(coef, pieces[offset]))
    return template(coef, order, dense, pieces[last])


def solution(mesh):
    placed = (
        P("subj", None, "slab"),
        P("subj", None, None, "slab"),
        P("subj", "slab"),
        P("subj"),
        P(),
        P("slab"),
    )
    subj, slab = mesh.shape["subj"], mesh.shape["slab"]

    def body(*args):
        return on_device(subj, slab, *args)

    return jax.shard_map(body, mesh=mesh, in_specs=placed, out_specs=P(), check_vma=False)
```

```python
import functools

import jax
import jax.numpy as jnp
from jax import lax
from jax.experimental import pallas as pl
from jax.experimental.pallas import tpu as pltpu
from jax.sharding import PartitionSpec as P

GRID_DEV = 1024
LANES = 128
SPLIT = 32
TILE = 256


def exchange(value, axis, size, bit):
    return lax.ppermute(value, axis, [(i, i ^ bit) for i in range(size)])


def exchange_by_core(value, subj, slab, even, odd):
    pairs = [(i * slab + j, (i ^ (odd if j & 1 else even)) * slab + j) for i in range(subj) for j in range(slab)]
    return lax.ppermute(value, ("subj", "slab"), pairs)


def sums_kernel(
    subjects,
    chunk,
    rotation_hbm,
    fod_hbm,
    modulation_hbm,
    ids_hbm,
    study_hbm,
    out_ref,
    rotation,
    fod,
    modulation,
    ids,
    study,
    weighted,
    partial,
    big_sem,
    small_sem,
):
    coef, _, rows, _ = rotation.shape
    small = [
        pltpu.make_async_copy(ids_hbm, ids, small_sem.at[0]),
        pltpu.make_async_copy(study_hbm, study, small_sem.at[1]),
        pltpu.make_async_copy(modulation_hbm, modulation, small_sem.at[2]),
        pltpu.make_async_copy(fod_hbm, fod, small_sem.at[3]),
    ]
    for copy in small:
        copy.start()

    def big(step):
        part = pl.ds(step * chunk, chunk)
        return pltpu.make_async_copy(rotation_hbm.at[part], rotation.at[part], big_sem.at[step])

    for step in range(coef // chunk):
        big(step).start(priority=1)
    for copy in small:
        copy.wait()

    subject = lax.broadcasted_iota(jnp.int32, (rows, LANES), 0) % subjects
    factor = jnp.zeros((rows, LANES), jnp.float32)
    for s in range(subjects):
        factor = jnp.where(subject == s, study[ids[s]], factor)
    weight = modulation[...] * factor
    partial[pl.ds(coef * rows, rows)] = weight
    for k in range(coef):
        weighted[k] = fod[k].astype(jnp.float32) * weight

    @pl.loop(0, coef // chunk)
    def _(step):
        big(step).wait()
        total = [jnp.zeros((rows, LANES), jnp.float32) for _ in range(chunk)]
        for k in range(coef):
            term = weighted[k]
            for c in range(chunk):
                total[c] += rotation[step * chunk + c, k].astype(jnp.float32) * term
        for c in range(chunk):
            partial[pl.ds(pl.multiple_of((step * chunk + c) * rows, rows), rows)] = total[c]

    count = out_ref.shape[0]
    out = partial[pl.ds(0, count, stride=subjects)]
    for s in range(1, subjects):
        out += partial[pl.ds(s, count, stride=subjects)]
    out_ref[...] = out


def local_sums(fod, rotation, modulation, subject_ids, subject_weight):
    subjects, coef, voxels = fod.shape
    blocks = voxels // LANES
    rows = blocks * subjects
    chunk = next(n for n in (5, 4, 3, 2, 1) if coef % n == 0)
    turned = rotation.transpose(1, 2, 0, 3).reshape(coef, coef, subjects, blocks, LANES)
    turned = turned.transpose(0, 1, 3, 2, 4).reshape(coef, coef, rows, LANES)
    fod = fod.transpose(1, 0, 2).reshape(coef, subjects, blocks, LANES).transpose(0, 2, 1, 3).reshape(coef, rows, LANES)
    modulation = modulation.reshape(subjects, blocks, LANES).transpose(1, 0, 2).reshape(rows, LANES)
    return pl.pallas_call(
        functools.partial(sums_kernel, subjects, chunk),
        out_shape=pltpu.VMEM(((coef + 1) * blocks, LANES), jnp.float32),
        in_specs=[pl.BlockSpec(memory_space=pl.ANY)] * 5,
        out_specs=pl.BlockSpec(memory_space=pltpu.VMEM),
        scratch_shapes=[
            pltpu.VMEM(turned.shape, turned.dtype),
            pltpu.VMEM(fod.shape, fod.dtype),
            pltpu.VMEM(modulation.shape, jnp.float32),
            pltpu.SMEM(subject_ids.shape, jnp.int32),
            pltpu.SMEM(subject_weight.shape, jnp.float32),
            pltpu.VMEM(fod.shape, jnp.float32),
            pltpu.VMEM(((coef + 1) * rows, LANES), jnp.float32),
            pltpu.SemaphoreType.DMA((coef // chunk,)),
            pltpu.SemaphoreType.DMA((4,)),
        ],
        compiler_params=pltpu.CompilerParams(vmem_limit_bytes=32 << 20),
        name="local_sums",
    )(*[pltpu.with_memory_space_constraint(x, pltpu.HBM) for x in (turned, fod, modulation, subject_ids, subject_weight)])


def finish_kernel(coef, terms, *refs):
    parts, (cells_ref, out_ref, total) = refs[:terms], refs[terms:]
    rows, voxels = out_ref.shape
    blocks = voxels // LANES
    values = [part[...] for part in parts]
    while len(values) > 1:
        values = [values[i] + values[i + 1] for i in range(0, len(values), 2)]
    total[pl.ds(0, parts[0].shape[0])] = values[0]
    row = lax.broadcasted_iota(jnp.int32, (rows, LANES), 0)
    for block in range(blocks):
        numer = total[pl.ds(block, rows, stride=blocks)]
        denom = total[pl.ds(coef * blocks + block, 1)]
        cells = cells_ref[pl.ds(block, 1)]
        high, low = (cells // SPLIT).astype(jnp.float32), (cells % SPLIT).astype(jnp.float32)
        value = jnp.where(row < coef, numer / denom, jnp.where(row == coef, high, jnp.where(row == coef + 1, low, 0.0)))
        out_ref[:, pl.ds(block * LANES, LANES)] = value.astype(jnp.bfloat16)


def finish(parts, cells, coef):
    blocks = cells.shape[0] // LANES
    rows = -(-(coef + 2) // 8) * 8
    return pl.pallas_call(
        functools.partial(finish_kernel, coef, len(parts)),
        out_shape=pltpu.VMEM((rows, cells.shape[0]), jnp.bfloat16),
        in_specs=[pl.BlockSpec(memory_space=pltpu.VMEM)] * (len(parts) + 1),
        out_specs=pl.BlockSpec(memory_space=pltpu.VMEM),
        scratch_shapes=[pltpu.VMEM((rows * blocks, LANES), jnp.float32)],
        compiler_params=pltpu.CompilerParams(vmem_limit_bytes=16 << 20),
        name="finish",
    )(*parts, cells.reshape(blocks, LANES))


def dense_of(coef, compact):
    voxels = compact.shape[1]
    high = compact[coef : coef + 1].astype(jnp.float32)
    low = compact[coef + 1 : coef + 2].astype(jnp.float32)
    cells = (high * SPLIT + low).astype(jnp.int32)
    tiles = []
    for start in range(0, GRID_DEV, TILE):
        first = max(start - (GRID_DEV - voxels), 0) // TILE * TILE
        last = min(start + TILE, voxels)
        hit = lax.broadcasted_iota(jnp.int32, (TILE, last - first), 0) + start == cells[:, first:last]
        onehot = jnp.where(hit, 1.0, 0.0).astype(jnp.bfloat16)
        tiles.append(
            lax.dot_general(compact[:, first:last], onehot, (((1,), (1,)), ((), ())), preferred_element_type=jnp.float32)
        )
    return jnp.concatenate(tiles, axis=1)[:coef].astype(jnp.bfloat16)


def place_kernel(coef, compact_ref, out_ref):
    out_ref[...] = dense_of(coef, compact_ref[...])


def place(coef, compact):
    return pl.pallas_call(
        functools.partial(place_kernel, coef),
        out_shape=pltpu.VMEM((coef, GRID_DEV), jnp.bfloat16),
        in_specs=[pl.BlockSpec(memory_space=pltpu.VMEM)],
        out_specs=pl.BlockSpec(memory_space=pltpu.VMEM),
        cost_estimate=pl.CostEstimate(flops=2 * coef * compact.shape[1] * GRID_DEV, bytes_accessed=1 << 18, transcendentals=0),
        compiler_params=pltpu.CompilerParams(vmem_limit_bytes=32 << 20),
        name="place",
    )(compact)


def template_kernel(coef, order, *refs):
    *ready, compact_ref, out_ref, last, sem = refs
    index = lax.axis_index("slab")

    def write(i, ref):
        columns = pl.ds(pl.multiple_of((index ^ order[i]) * GRID_DEV, GRID_DEV), GRID_DEV)
        return pltpu.make_async_copy(ref, out_ref.at[:, columns], sem.at[i])

    copies = [write(i, ref) for i, ref in enumerate(ready)]
    for copy in copies:
        copy.start()
    last[...] = dense_of(coef, compact_ref[...])
    copies.append(write(len(ready), last))
    copies[-1].start()
    for copy in copies:
        copy.wait()


def template(coef, order, ready, compact):
    return pl.pallas_call(
        functools.partial(template_kernel, coef, order),
        out_shape=jax.ShapeDtypeStruct((coef, len(order) * GRID_DEV), jnp.bfloat16),
        in_specs=[pl.BlockSpec(memory_space=pltpu.VMEM)] * len(order),
        out_specs=pl.BlockSpec(memory_space=pl.ANY),
        scratch_shapes=[pltpu.VMEM((coef, GRID_DEV), jnp.bfloat16), pltpu.SemaphoreType.DMA((len(order),))],
        compiler_params=pltpu.CompilerParams(vmem_limit_bytes=32 << 20),
        name="template",
    )(*ready, compact)


def on_device(subj, slab, fod, rotation, modulation, subject_ids, subject_weight, voxel_cell_index):
    coef = fod.shape[1]
    mine = local_sums(fod, rotation, modulation, subject_ids, subject_weight)
    count = subj.bit_length() - 1
    bits = [1 << n for n in range(count)]
    even, odd = [bits[-1], *bits[:-1]], [bits[-2], *bits[:-2], bits[-1]]
    for one, other in zip(even[:-2], odd[:-2]):
        mine = mine + exchange_by_core(mine, subj, slab, one, other)
    parts = [mine]
    for pick in ((0,), (1,), (0, 1)):
        offsets = [sum(order[-2:][n] for n in pick) for order in (even, odd)]
        parts.append(exchange_by_core(mine, subj, slab, *offsets))
    own = finish(parts, voxel_cell_index, coef)
    pieces = {0: own}
    for offset in reversed(range(1, slab)):
        pieces[offset] = exchange(own, "slab", slab, offset)
    last = slab // 2
    order = [o for o in sorted(pieces) if o != last] + [last]
    dense = []
    for offset in order[:-1]:
        dense.append(place(coef, pieces[offset]))
    return template(coef, order, dense, pieces[last])


def solution(mesh):
    placed = (
        P("subj", None, "slab"),
        P("subj", None, None, "slab"),
        P("subj", "slab"),
        P("subj"),
        P(),
        P("slab"),
    )
    subj, slab = mesh.shape["subj"], mesh.shape["slab"]

    def body(*args):
        return on_device(subj, slab, *args)

    return jax.shard_map(body, mesh=mesh, in_specs=placed, out_specs=P(), check_vma=False)
```

```python
import functools

import jax
import jax.numpy as jnp
from jax import lax
from jax.experimental import pallas as pl
from jax.experimental.pallas import tpu as pltpu
from jax.sharding import PartitionSpec as P

GRID_DEV = 1024
LANES = 128
SPLIT = 32
TILE = 256


def exchange(value, axis, size, bit):
    return lax.ppermute(value, axis, [(i, i ^ bit) for i in range(size)])


def exchange_by_core(value, subj, slab, even, odd):
    pairs = [(i * slab + j, (i ^ (odd if j & 1 else even)) * slab + j) for i in range(subj) for j in range(slab)]
    return lax.ppermute(value, ("subj", "slab"), pairs)


def sums_kernel(
    subjects,
    chunk,
    rotation_hbm,
    fod_hbm,
    modulation_hbm,
    ids_hbm,
    study_hbm,
    out_ref,
    rotation,
    fod,
    modulation,
    ids,
    study,
    weighted,
    partial,
    big_sem,
    small_sem,
):
    coef, _, rows, _ = rotation.shape
    small = [
        pltpu.make_async_copy(ids_hbm, ids, small_sem.at[0]),
        pltpu.make_async_copy(study_hbm, study, small_sem.at[1]),
        pltpu.make_async_copy(modulation_hbm, modulation, small_sem.at[2]),
        pltpu.make_async_copy(fod_hbm, fod, small_sem.at[3]),
    ]

    def big(step):
        part = pl.ds(step * chunk, chunk)
        return pltpu.make_async_copy(rotation_hbm.at[part], rotation.at[part], big_sem.at[step])

    for step in range(coef // chunk):
        big(step).start(priority=1)
    for copy in small:
        copy.start()
    for copy in small:
        copy.wait()

    subject = lax.broadcasted_iota(jnp.int32, (rows, LANES), 0) % subjects
    factor = jnp.zeros((rows, LANES), jnp.float32)
    for s in range(subjects):
        factor = jnp.where(subject == s, study[ids[s]], factor)
    weight = modulation[...] * factor
    partial[pl.ds(coef * rows, rows)] = weight
    for k in range(coef):
        weighted[k] = fod[k].astype(jnp.float32) * weight

    @pl.loop(0, coef // chunk)
    def _(step):
        big(step).wait()
        total = [jnp.zeros((rows, LANES), jnp.float32) for _ in range(chunk)]
        for k in range(coef):
            term = weighted[k]
            for c in range(chunk):
                total[c] += rotation[step * chunk + c, k].astype(jnp.float32) * term
        for c in range(chunk):
            partial[pl.ds(pl.multiple_of((step * chunk + c) * rows, rows), rows)] = total[c]

    count = out_ref.shape[0]
    out = partial[pl.ds(0, count, stride=subjects)]
    for s in range(1, subjects):
        out += partial[pl.ds(s, count, stride=subjects)]
    out_ref[...] = out


def local_sums(fod, rotation, modulation, subject_ids, subject_weight):
    subjects, coef, voxels = fod.shape
    blocks = voxels // LANES
    rows = blocks * subjects
    chunk = next(n for n in (5, 4, 3, 2, 1) if coef % n == 0)
    turned = rotation.transpose(1, 2, 0, 3).reshape(coef, coef, subjects, blocks, LANES)
    turned = turned.transpose(0, 1, 3, 2, 4).reshape(coef, coef, rows, LANES)
    fod = fod.transpose(1, 0, 2).reshape(coef, subjects, blocks, LANES).transpose(0, 2, 1, 3).reshape(coef, rows, LANES)
    modulation = modulation.reshape(subjects, blocks, LANES).transpose(1, 0, 2).reshape(rows, LANES)
    return pl.pallas_call(
        functools.partial(sums_kernel, subjects, chunk),
        out_shape=pltpu.VMEM(((coef + 1) * blocks, LANES), jnp.float32),
        in_specs=[pl.BlockSpec(memory_space=pl.ANY)] * 5,
        out_specs=pl.BlockSpec(memory_space=pltpu.VMEM),
        scratch_shapes=[
            pltpu.VMEM(turned.shape, turned.dtype),
            pltpu.VMEM(fod.shape, fod.dtype),
            pltpu.VMEM(modulation.shape, jnp.float32),
            pltpu.SMEM(subject_ids.shape, jnp.int32),
            pltpu.SMEM(subject_weight.shape, jnp.float32),
            pltpu.VMEM(fod.shape, jnp.float32),
            pltpu.VMEM(((coef + 1) * rows, LANES), jnp.float32),
            pltpu.SemaphoreType.DMA((coef // chunk,)),
            pltpu.SemaphoreType.DMA((4,)),
        ],
        compiler_params=pltpu.CompilerParams(vmem_limit_bytes=32 << 20),
        name="local_sums",
    )(*[pltpu.with_memory_space_constraint(x, pltpu.HBM) for x in (turned, fod, modulation, subject_ids, subject_weight)])


def finish_kernel(coef, terms, *refs):
    parts, (cells_ref, out_ref, total) = refs[:terms], refs[terms:]
    rows, voxels = out_ref.shape
    blocks = voxels // LANES
    values = [part[...] for part in parts]
    while len(values) > 1:
        values = [values[i] + values[i + 1] for i in range(0, len(values), 2)]
    total[pl.ds(0, parts[0].shape[0])] = values[0]
    row = lax.broadcasted_iota(jnp.int32, (rows, LANES), 0)
    for block in range(blocks):
        numer = total[pl.ds(block, rows, stride=blocks)]
        denom = total[pl.ds(coef * blocks + block, 1)]
        cells = cells_ref[pl.ds(block, 1)]
        high, low = (cells // SPLIT).astype(jnp.float32), (cells % SPLIT).astype(jnp.float32)
        value = jnp.where(row < coef, numer / denom, jnp.where(row == coef, high, jnp.where(row == coef + 1, low, 0.0)))
        out_ref[:, pl.ds(block * LANES, LANES)] = value.astype(jnp.bfloat16)


def finish(parts, cells, coef):
    blocks = cells.shape[0] // LANES
    rows = -(-(coef + 2) // 8) * 8
    return pl.pallas_call(
        functools.partial(finish_kernel, coef, len(parts)),
        out_shape=pltpu.VMEM((rows, cells.shape[0]), jnp.bfloat16),
        in_specs=[pl.BlockSpec(memory_space=pltpu.VMEM)] * (len(parts) + 1),
        out_specs=pl.BlockSpec(memory_space=pltpu.VMEM),
        scratch_shapes=[pltpu.VMEM((rows * blocks, LANES), jnp.float32)],
        compiler_params=pltpu.CompilerParams(vmem_limit_bytes=16 << 20),
        name="finish",
    )(*parts, cells.reshape(blocks, LANES))


def dense_of(coef, compact):
    voxels = compact.shape[1]
    high = compact[coef : coef + 1].astype(jnp.float32)
    low = compact[coef + 1 : coef + 2].astype(jnp.float32)
    cells = (high * SPLIT + low).astype(jnp.int32).astype(jnp.int16)
    tiles = []
    for start in range(0, GRID_DEV, TILE):
        first = max(start - (GRID_DEV - voxels), 0) // TILE * TILE
        last = min(start + TILE, voxels)
        hit = lax.broadcasted_iota(jnp.int16, (TILE, last - first), 0) + jnp.int16(start) == cells[:, first:last]
        onehot = jnp.where(hit, jnp.bfloat16(1), jnp.bfloat16(0))
        tiles.append(
            lax.dot_general(compact[:, first:last], onehot, (((1,), (1,)), ((), ())), preferred_element_type=jnp.float32)
        )
    return jnp.concatenate(tiles, axis=1)[:coef].astype(jnp.bfloat16)


def place_kernel(coef, compact_ref, out_ref):
    out_ref[...] = dense_of(coef, compact_ref[...])


def place(coef, compact):
    return pl.pallas_call(
        functools.partial(place_kernel, coef),
        out_shape=pltpu.VMEM((coef, GRID_DEV), jnp.bfloat16),
        in_specs=[pl.BlockSpec(memory_space=pltpu.VMEM)],
        out_specs=pl.BlockSpec(memory_space=pltpu.VMEM),
        cost_estimate=pl.CostEstimate(flops=2 * coef * compact.shape[1] * GRID_DEV, bytes_accessed=1 << 18, transcendentals=0),
        compiler_params=pltpu.CompilerParams(vmem_limit_bytes=32 << 20),
        name="place",
    )(compact)


def template_kernel(coef, order, *refs):
    *ready, compact_ref, out_ref, last, sem = refs
    index = lax.axis_index("slab")

    def write(i, ref):
        columns = pl.ds(pl.multiple_of((index ^ order[i]) * GRID_DEV, GRID_DEV), GRID_DEV)
        return pltpu.make_async_copy(ref, out_ref.at[:, columns], sem.at[i])

    copies = [write(i, ref) for i, ref in enumerate(ready)]
    for copy in copies:
        copy.start()
    last[...] = dense_of(coef, compact_ref[...])
    copies.append(write(len(ready), last))
    copies[-1].start()
    for copy in copies:
        copy.wait()


def template(coef, order, ready, compact):
    return pl.pallas_call(
        functools.partial(template_kernel, coef, order),
        out_shape=jax.ShapeDtypeStruct((coef, len(order) * GRID_DEV), jnp.bfloat16),
        in_specs=[pl.BlockSpec(memory_space=pltpu.VMEM)] * len(order),
        out_specs=pl.BlockSpec(memory_space=pl.ANY),
        scratch_shapes=[pltpu.VMEM((coef, GRID_DEV), jnp.bfloat16), pltpu.SemaphoreType.DMA((len(order),))],
        compiler_params=pltpu.CompilerParams(vmem_limit_bytes=32 << 20),
        name="template",
    )(*ready, compact)


def on_device(subj, slab, fod, rotation, modulation, subject_ids, subject_weight, voxel_cell_index):
    coef = fod.shape[1]
    mine = local_sums(fod, rotation, modulation, subject_ids, subject_weight)
    count = subj.bit_length() - 1
    bits = [1 << n for n in range(count)]
    even, odd = [bits[-1], *bits[:-1]], [bits[-2], *bits[:-2], bits[-1]]
    for one, other in zip(even[:-2], odd[:-2]):
        mine = mine + exchange_by_core(mine, subj, slab, one, other)
    parts = [mine]
    for pick in ((0,), (1,), (0, 1)):
        offsets = [sum(order[-2:][n] for n in pick) for order in (even, odd)]
        parts.append(exchange_by_core(mine, subj, slab, *offsets))
    own = finish(parts, voxel_cell_index, coef)
    pieces = {0: own}
    for offset in reversed(range(1, slab)):
        pieces[offset] = exchange(own, "slab", slab, offset)
    last = slab // 2
    order = [o for o in sorted(pieces) if o != last] + [last]
    dense = []
    for offset in order[:-1]:
        dense.append(place(coef, pieces[offset]))
    return template(coef, order, dense, pieces[last])


def solution(mesh):
    placed = (
        P("subj", None, "slab"),
        P("subj", None, None, "slab"),
        P("subj", "slab"),
        P("subj"),
        P(),
        P("slab"),
    )
    subj, slab = mesh.shape["subj"], mesh.shape["slab"]

    def body(*args):
        return on_device(subj, slab, *args)

    return jax.shard_map(body, mesh=mesh, in_specs=placed, out_specs=P(), check_vma=False)
```

```python
import functools

import jax
import jax.numpy as jnp
from jax import lax
from jax.experimental import pallas as pl
from jax.experimental.pallas import tpu as pltpu
from jax.sharding import PartitionSpec as P

GRID_DEV = 1024
LANES = 128
SPLIT = 32
TILE = 256


def exchange(value, axis, size, bit):
    return lax.ppermute(value, axis, [(i, i ^ bit) for i in range(size)])


def exchange_by_core(value, subj, slab, even, odd):
    pairs = [(i * slab + j, (i ^ (odd if j & 1 else even)) * slab + j) for i in range(subj) for j in range(slab)]
    return lax.ppermute(value, ("subj", "slab"), pairs)


def sums_kernel(
    subjects,
    chunk,
    rotation_hbm,
    fod_hbm,
    modulation_hbm,
    ids_hbm,
    study_hbm,
    out_ref,
    rotation,
    fod,
    modulation,
    ids,
    study,
    weighted,
    partial,
    big_sem,
    small_sem,
):
    coef, _, rows, _ = rotation.shape
    small = [
        pltpu.make_async_copy(ids_hbm, ids, small_sem.at[0]),
        pltpu.make_async_copy(study_hbm, study, small_sem.at[1]),
        pltpu.make_async_copy(modulation_hbm, modulation, small_sem.at[2]),
        pltpu.make_async_copy(fod_hbm, fod, small_sem.at[3]),
    ]
    for copy in small:
        copy.start()

    def big(step):
        part = pl.ds(step * chunk, chunk)
        return pltpu.make_async_copy(rotation_hbm.at[part], rotation.at[part], big_sem.at[step])

    for step in range(coef // chunk):
        big(step).start(priority=1)
    for copy in small:
        copy.wait()

    subject = lax.broadcasted_iota(jnp.int32, (rows, LANES), 0) % subjects
    factor = jnp.zeros((rows, LANES), jnp.float32)
    for s in range(subjects):
        factor = jnp.where(subject == s, study[ids[s]], factor)
    weight = modulation[...] * factor
    partial[pl.ds(coef * rows, rows)] = weight
    for k in range(coef):
        weighted[k] = fod[k].astype(jnp.float32) * weight

    @pl.loop(0, coef // chunk)
    def _(step):
        big(step).wait()
        total = [jnp.zeros((rows, LANES), jnp.float32) for _ in range(chunk)]
        for k in range(coef):
            term = weighted[k]
            for c in range(chunk):
                total[c] += rotation[step * chunk + c, k].astype(jnp.float32) * term
        for c in range(chunk):
            partial[pl.ds(pl.multiple_of((step * chunk + c) * rows, rows), rows)] = total[c]

    count = out_ref.shape[0]
    out = partial[pl.ds(0, count, stride=subjects)]
    for s in range(1, subjects):
        out += partial[pl.ds(s, count, stride=subjects)]
    out_ref[...] = out


def local_sums(fod, rotation, modulation, subject_ids, subject_weight):
    subjects, coef, voxels = fod.shape
    blocks = voxels // LANES
    rows = blocks * subjects
    chunk = next(n for n in (5, 4, 3, 2, 1) if coef % n == 0)
    turned = rotation.transpose(1, 2, 0, 3).reshape(coef, coef, subjects, blocks, LANES)
    turned = turned.transpose(0, 1, 3, 2, 4).reshape(coef, coef, rows, LANES)
    fod = fod.transpose(1, 0, 2).reshape(coef, subjects, blocks, LANES).transpose(0, 2, 1, 3).reshape(coef, rows, LANES)
    modulation = modulation.reshape(subjects, blocks, LANES).transpose(1, 0, 2).reshape(rows, LANES)
    return pl.pallas_call(
        functools.partial(sums_kernel, subjects, chunk),
        out_shape=pltpu.VMEM(((coef + 1) * blocks, LANES), jnp.float32),
        in_specs=[pl.BlockSpec(memory_space=pl.ANY)] * 5,
        out_specs=pl.BlockSpec(memory_space=pltpu.VMEM),
        scratch_shapes=[
            pltpu.VMEM(turned.shape, turned.dtype),
            pltpu.VMEM(fod.shape, fod.dtype),
            pltpu.VMEM(modulation.shape, jnp.float32),
            pltpu.SMEM(subject_ids.shape, jnp.int32),
            pltpu.SMEM(subject_weight.shape, jnp.float32),
            pltpu.VMEM(fod.shape, jnp.float32),
            pltpu.VMEM(((coef + 1) * rows, LANES), jnp.float32),
            pltpu.SemaphoreType.DMA((coef // chunk,)),
            pltpu.SemaphoreType.DMA((4,)),
        ],
        compiler_params=pltpu.CompilerParams(vmem_limit_bytes=32 << 20),
        name="local_sums",
    )(*[pltpu.with_memory_space_constraint(x, pltpu.HBM) for x in (turned, fod, modulation, subject_ids, subject_weight)])


def finish_kernel(coef, terms, *refs):
    parts, (cells_ref, out_ref, total) = refs[:terms], refs[terms:]
    rows, voxels = out_ref.shape
    blocks = voxels // LANES
    values = [part[...] for part in parts]
    while len(values) > 1:
        values = [values[i] + values[i + 1] for i in range(0, len(values), 2)]
    total[pl.ds(0, parts[0].shape[0])] = values[0]
    row = lax.broadcasted_iota(jnp.int32, (rows, LANES), 0)
    for block in range(blocks):
        numer = total[pl.ds(block, rows, stride=blocks)]
        denom = total[pl.ds(coef * blocks + block, 1)]
        cells = cells_ref[pl.ds(block, 1)]
        high, low = (cells // SPLIT).astype(jnp.float32), (cells % SPLIT).astype(jnp.float32)
        value = jnp.where(row < coef, numer / denom, jnp.where(row == coef, high, jnp.where(row == coef + 1, low, 0.0)))
        out_ref[:, pl.ds(block * LANES, LANES)] = value.astype(jnp.bfloat16)


def finish(parts, cells, coef):
    blocks = cells.shape[0] // LANES
    rows = -(-(coef + 2) // 8) * 8
    return pl.pallas_call(
        functools.partial(finish_kernel, coef, len(parts)),
        out_shape=pltpu.VMEM((rows, cells.shape[0]), jnp.bfloat16),
        in_specs=[pl.BlockSpec(memory_space=pltpu.VMEM)] * (len(parts) + 1),
        out_specs=pl.BlockSpec(memory_space=pltpu.VMEM),
        scratch_shapes=[pltpu.VMEM((rows * blocks, LANES), jnp.float32)],
        compiler_params=pltpu.CompilerParams(vmem_limit_bytes=16 << 20),
        name="finish",
    )(*parts, cells.reshape(blocks, LANES))


def dense_tiles(coef, compact):
    voxels = compact.shape[1]
    high = compact[coef : coef + 1].astype(jnp.float32)
    low = compact[coef + 1 : coef + 2].astype(jnp.float32)
    cells = (high * SPLIT + low).astype(jnp.int32)
    for start in range(0, GRID_DEV, TILE):
        first = max(start - (GRID_DEV - voxels), 0) // TILE * TILE
        last = min(start + TILE, voxels)
        hit = lax.broadcasted_iota(jnp.int32, (TILE, last - first), 0) + start == cells[:, first:last]
        onehot = jnp.where(hit, 1.0, 0.0).astype(jnp.bfloat16)
        dense = lax.dot_general(compact[:, first:last], onehot, (((1,), (1,)), ((), ())), preferred_element_type=jnp.float32)
        yield start, dense[:coef].astype(jnp.bfloat16)


def place_kernel(coef, compact_ref, out_ref):
    for start, tile in dense_tiles(coef, compact_ref[...]):
        out_ref[:, pl.ds(start, TILE)] = tile


def place(coef, compact):
    return pl.pallas_call(
        functools.partial(place_kernel, coef),
        out_shape=pltpu.VMEM((coef, GRID_DEV), jnp.bfloat16),
        in_specs=[pl.BlockSpec(memory_space=pltpu.VMEM)],
        out_specs=pl.BlockSpec(memory_space=pltpu.VMEM),
        cost_estimate=pl.CostEstimate(flops=2 * coef * compact.shape[1] * GRID_DEV, bytes_accessed=1 << 18, transcendentals=0),
        compiler_params=pltpu.CompilerParams(vmem_limit_bytes=32 << 20),
        name="place",
    )(compact)


def template_kernel(coef, order, *refs):
    *ready, compact_ref, out_ref, last, sem = refs
    index = lax.axis_index("slab")

    def write(i, ref):
        columns = pl.ds(pl.multiple_of((index ^ order[i]) * GRID_DEV, GRID_DEV), GRID_DEV)
        return pltpu.make_async_copy(ref, out_ref.at[:, columns], sem.at[i])

    copies = [write(i, ref) for i, ref in enumerate(ready)]
    for copy in copies:
        copy.start()
    base = pl.multiple_of((index ^ order[-1]) * GRID_DEV, GRID_DEV)
    for n, (start, tile) in enumerate(dense_tiles(coef, compact_ref[...])):
        here = pl.ds(start, TILE)
        last[:, here] = tile
        there = out_ref.at[:, pl.ds(pl.multiple_of(base + start, TILE), TILE)]
        copies.append(pltpu.make_async_copy(last.at[:, here], there, sem.at[len(ready) + n]))
        copies[-1].start()
    for copy in copies:
        copy.wait()


def template(coef, order, ready, compact):
    return pl.pallas_call(
        functools.partial(template_kernel, coef, order),
        out_shape=jax.ShapeDtypeStruct((coef, len(order) * GRID_DEV), jnp.bfloat16),
        in_specs=[pl.BlockSpec(memory_space=pltpu.VMEM)] * len(order),
        out_specs=pl.BlockSpec(memory_space=pl.ANY),
        scratch_shapes=[pltpu.VMEM((coef, GRID_DEV), jnp.bfloat16), pltpu.SemaphoreType.DMA((len(ready) + GRID_DEV // TILE,))],
        compiler_params=pltpu.CompilerParams(vmem_limit_bytes=32 << 20),
        name="template",
    )(*ready, compact)


def on_device(subj, slab, fod, rotation, modulation, subject_ids, subject_weight, voxel_cell_index):
    coef = fod.shape[1]
    mine = local_sums(fod, rotation, modulation, subject_ids, subject_weight)
    count = subj.bit_length() - 1
    bits = [1 << n for n in range(count)]
    even, odd = [bits[-1], *bits[:-1]], [bits[-2], *bits[:-2], bits[-1]]
    for one, other in zip(even[:-2], odd[:-2]):
        mine = mine + exchange_by_core(mine, subj, slab, one, other)
    parts = [mine]
    for pick in ((0,), (1,), (0, 1)):
        offsets = [sum(order[-2:][n] for n in pick) for order in (even, odd)]
        parts.append(exchange_by_core(mine, subj, slab, *offsets))
    own = finish(parts, voxel_cell_index, coef)
    pieces = {0: own}
    for offset in reversed(range(1, slab)):
        pieces[offset] = exchange(own, "slab", slab, offset)
    last = slab // 2
    order = [o for o in sorted(pieces) if o != last] + [last]
    dense = []
    for offset in order[:-1]:
        dense.append(place(coef, pieces[offset]))
    return template(coef, order, dense, pieces[last])


def solution(mesh):
    placed = (
        P("subj", None, "slab"),
        P("subj", None, None, "slab"),
        P("subj", "slab"),
        P("subj"),
        P(),
        P("slab"),
    )
    subj, slab = mesh.shape["subj"], mesh.shape["slab"]

    def body(*args):
        return on_device(subj, slab, *args)

    return jax.shard_map(body, mesh=mesh, in_specs=placed, out_specs=P(), check_vma=False)
```
